128 devices in a mesh: lat: 16 (over z_lo, y, core), lon: 8 (over z_hi, x).
Axes of the slice: x: 4, y: 4, z: 4 (z_hi: 2, z_lo: 2; z = z_hi * 2 + z_lo), core: 2. Of those that a mesh axis runs over, the one named last changes fastest.
Arguments:
- tokens: bfloat16 [4, 128, 256, 1024], P(None, 'lat', 'lon'), may hold values from -6 to 6
- qkv_weight: bfloat16 [3072, 1024], P(('lat', 'lon')), may hold values from -0.1875 to 0.1875
- proj_weight: bfloat16 [1024, 1024], P(('lat', 'lon')), may hold values from -0.1875 to 0.1875
- up_weight: bfloat16 [4096, 1024], P(('lat', 'lon')), may hold values from -0.1875 to 0.1875
- down_weight: bfloat16 [4096, 1024], P(('lat', 'lon')), may hold values from -0.09375 to 0.09375
- bias_table: float32 [225, 16], replicated, may hold values from -3 to 220, as said below
- sea_mask: int32 [128, 256], replicated, may hold values 0 or 1
Outputs:
- block_out: bfloat16 [4, 128, 256, 1024], P(None, 'lat', 'lon')
The draws below stay inside these ranges and needn't reach their ends.
Inputs may be any that keep to these rules, and one draw needn't show every extreme that they name: `bias_table`: entry [o, h] is the bias of head h for the in-window offset numbered o as in the reference program.
All inputs are finite; a program needn't handle non-finite values.
Results may differ from the reference program's by a relative error of at most 0.012.
Values may be sent and summed in bfloat16 or wider, within the bound.
No kernel may reach another device: no remote copies, remote signals or barrier semaphores. Data moves between devices by JAX's collectives and lax.ppermute only.
A program may use at most 128 MiB of HBM per device.

```python
import jax
import jax.numpy as jnp
from jax import lax

D = 1024
HEADS = 16
MLP = 4096
BATCH = 4
RELPOS = 225
HEAD_DIM = 64
NLAT = 128
NLON = 256


def draw_bias_table(key, part):
    base_key, head_key = jax.random.split(jax.random.fold_in(key, 7))
    bias_rows = jnp.clip(jax.random.normal(base_key, (RELPOS, HEADS), jnp.float32), -3.0, 3.0)
    return bias_rows


def plant(values, stream_key, smallest, top_value):
    place = [jax.random.randint(jax.random.fold_in(stream_key, axis), (), 0, length) for axis, length in enumerate(values.shape)]
    main_axis = values.shape.index(max(values.shape))
    next_to = place[:main_axis] + [(place[main_axis] + 1) % values.shape[main_axis]] + place[main_axis + 1:]
    return values.at[tuple(place)].set(smallest).at[tuple(next_to)].set(top_value)


def shard_levels(rng, shape, pieces, least, top_value):
    level = 1.0
    for position, blocks in pieces:
        steps = jax.random.uniform(jax.random.fold_in(jax.random.fold_in(rng, 6), position), (blocks,), jnp.float32, least / len(pieces), top_value / len(pieces))
        level = level * jnp.repeat(jnp.exp(steps), shape[position] // blocks).reshape((-1,) + (1,) * (len(shape) - 1 - position))
    return level


def noise(rng, dims, deviation, reach, pieces=(), kind=jnp.bfloat16):
    drawn = jax.random.normal(rng, dims, jnp.float32) * deviation
    if len(pieces) > 0:
        drawn = shard_levels(rng, dims, pieces, -0.22, 0.18) * drawn
    return jnp.clip(drawn, min=-reach, max=reach).astype(kind)


def setup_inputs(seed: int = 0) -> dict:
    splits = jax.random.split(jax.random.key(seed), 8)
    return {
        "tokens": noise(splits[0], (BATCH, NLAT, NLON, D), 1.0, 6.0, ((1, 16), (2, 8))),
        "qkv_weight": noise(splits[1], (3 * D, D), D ** -0.5, 0.1875, ((0, 128),)),
        "proj_weight": noise(splits[2], (D, D), D ** -0.5, 0.1875, ((0, 128),)),
        "up_weight": noise(splits[3], (MLP, D), D ** -0.5, 0.1875, ((0, 128),)),
        "down_weight": noise(splits[4], (MLP, D), MLP ** -0.5, 0.09375, ((0, 128),)),
        "bias_table": draw_bias_table(jax.random.fold_in(splits[7], 71), 0),
        "sea_mask": plant((jax.random.randint(splits[6], (NLAT, NLON), 0, 4) < 3).astype(jnp.int32), jax.random.fold_in(splits[6], 1), 0, 1),
    }


def layer_norm(values):
    widened = values.astype(jnp.float32)
    centre = lax.optimization_barrier(jnp.mean(widened, axis=-1, keepdims=True))
    spread = lax.optimization_barrier(jnp.mean(jnp.square(widened - centre), axis=-1, keepdims=True))
    return ((widened - centre) * lax.rsqrt(spread + 1e-05)).astype(jnp.bfloat16)

def offsets_table():
    cell_ids = jnp.arange(64, dtype=jnp.int32)
    row_of = cell_ids // 8
    col_of = cell_ids % 8
    return (row_of[:, None] - row_of[None, :] + 7) * 15 + (col_of[:, None] - col_of[None, :] + 7)

def row_region(row_ids, total_rows):
    return jnp.where(row_ids < 4, 2, jnp.where(row_ids >= total_rows - 4, 1, 0)).astype(jnp.int32)

def reference(tokens, qkv_weight, proj_weight, up_weight, down_weight, bias_table, sea_mask):
    normed = layer_norm(tokens)
    rolled = jnp.roll(normed, (-4, -4), axis=(1, 2))
    sea_rolled = jnp.roll(sea_mask, (-4, -4), axis=(0, 1))
    pos_bias = jnp.transpose(bias_table[offsets_table()], (2, 0, 1))
    same_cell = jnp.eye(64, dtype=bool)
    windows_across = NLON // 8
    row_blocks = jnp.transpose(rolled.reshape(BATCH, NLAT // 8, 8, NLON, D), (1, 0, 2, 3, 4))
    sea_blocks = sea_rolled.reshape(NLAT // 8, 8, NLON)
    score_scale = HEAD_DIM ** (-0.5)

    def window_row(inputs):
        row_block, sea_rows, block_index = inputs
        projected = jnp.dot(row_block.reshape(-1, D), qkv_weight.T, preferred_element_type=jnp.float32).astype(jnp.bfloat16)
        windows = projected.reshape(BATCH, 8, windows_across, 8, 3 * D).transpose(0, 2, 1, 3, 4)
        windows = windows.reshape(BATCH, windows_across, 64, 3, HEADS, HEAD_DIM).astype(jnp.float32)
        queries = windows[:, :, :, 0]
        keys_here = windows[:, :, :, 1]
        values_here = windows[:, :, :, 2]
        scores = jnp.einsum('bsqhd,bskhd->bshqk', queries, keys_here) * score_scale + pos_bias[None, None]
        grid_rows = (block_index * 8 + 4 + jnp.arange(8, dtype=jnp.int32)) % NLAT
        region = jnp.repeat(row_region(grid_rows, NLAT), 8)
        sea_keep = sea_rows.reshape(8, windows_across, 8).transpose(1, 0, 2).reshape(windows_across, 64) == 1
        allowed = (region[:, None] == region[None, :])[None] & (sea_keep[:, None, :] | same_cell[None])
        scores = jnp.where(allowed[None, :, None], scores, -1e+30)
        row_top = lax.optimization_barrier(jnp.max(scores, axis=-1, keepdims=True))
        weights = jnp.exp(scores - row_top)
        attn_probs = (weights / lax.optimization_barrier(jnp.sum(weights, axis=-1, keepdims=True))).astype(jnp.bfloat16)
        context = jnp.einsum('bshqk,bskhd->bsqhd', attn_probs.astype(jnp.float32), values_here).astype(jnp.bfloat16)
        context = context.reshape(BATCH, windows_across, 8, 8, D).transpose(0, 2, 1, 3, 4)
        return context.reshape(BATCH, 8, NLON, D)
    contexts = lax.map(window_row, (row_blocks, sea_blocks, jnp.arange(NLAT // 8, dtype=jnp.int32)))
    context_grid = jnp.transpose(contexts, (1, 0, 2, 3, 4)).reshape(BATCH, NLAT, NLON, D)
    context_grid = jnp.roll(context_grid, (4, 4), axis=(1, 2))

    def finish(inputs):
        token_block, context_block = inputs
        attention_out = jnp.dot(context_block.reshape(-1, D), proj_weight.T, preferred_element_type=jnp.float32)
        attended = (token_block.reshape(-1, D).astype(jnp.float32) + attention_out).astype(jnp.bfloat16)
        normed_two = layer_norm(attended)
        hidden = jax.nn.gelu(jnp.dot(normed_two, up_weight.T, preferred_element_type=jnp.float32)).astype(jnp.bfloat16)
        result = attended.astype(jnp.float32) + jnp.dot(hidden, down_weight, preferred_element_type=jnp.float32)
        return result.astype(jnp.bfloat16).reshape(token_block.shape)
    token_rows = jnp.transpose(tokens.reshape(BATCH, NLAT // 8, 8, NLON, D), (1, 0, 2, 3, 4))
    context_rows = jnp.transpose(context_grid.reshape(BATCH, NLAT // 8, 8, NLON, D), (1, 0, 2, 3, 4))
    finished = lax.map(finish, (token_rows, context_rows))
    return jnp.transpose(finished, (1, 0, 2, 3, 4)).reshape(BATCH, NLAT, NLON, D)
```

```python
import math

import jax
import jax.numpy as jnp
from jax import lax
from jax.sharding import Mesh
from jax.sharding import PartitionSpec as P


def from_behind(value, axis, steps):
    count = math.prod(lax.axis_size(a) for a in axis)
    pairs = [(source, (source + steps) % count) for source in range(count)]
    return lax.ppermute(value, axis, pairs)


AXES = ("zl", "y", "c", "zh", "x")
SIZES = (2, 4, 2, 2, 4)
LAT = ("zl", "y", "c")
LON = ("zh", "x")
TORUS = ("zh", "zl", "y", "x", "c")
TO_LOGICAL = tuple(TORUS.index(a) for a in AXES)


def gather_weights(arrays):
    rows = [a.shape[0] for a in arrays]
    width = arrays[0].shape[1]
    both = jnp.concatenate(arrays, axis=0)
    every = lax.all_gather(both, TORUS, axis=0, tiled=True)
    every = every.reshape(tuple(SIZES[AXES.index(a)] for a in TORUS) + both.shape)
    out, at = [], 0
    for count in rows:
        part = every[..., at : at + count, :]
        at += count
        out.append(part.transpose(TO_LOGICAL + (5, 6)).reshape(-1, width))
    return out


def layer_norm(values):
    widened = values.astype(jnp.float32)
    centre = jnp.mean(widened, axis=-1, keepdims=True)
    spread = jnp.mean(jnp.square(widened - centre), axis=-1, keepdims=True)
    return ((widened - centre) * lax.rsqrt(spread + 1e-05)).astype(jnp.bfloat16)


def offsets_table():
    cell_ids = jnp.arange(64, dtype=jnp.int32)
    row_of = cell_ids // 8
    col_of = cell_ids % 8
    return (row_of[:, None] - row_of[None, :] + 7) * 15 + (col_of[:, None] - col_of[None, :] + 7)


def row_region(row_ids, total_rows):
    return jnp.where(row_ids < 4, 2, jnp.where(row_ids >= total_rows - 4, 1, 0)).astype(jnp.int32)


def window_attention(queries, pair_cells, row_start, col_start, sea_mask, pos_bias):
    batch_size, row_count, col_count, feat_width = queries.shape
    head_count = pos_bias.shape[0]
    head_size = feat_width // head_count
    lat_cells, lon_cells = sea_mask.shape
    down_count = row_count // 8
    across_count = col_count // 8
    window_count = down_count * across_count

    def to_windows(values):
        last_dim = values.shape[-1]
        shaped = values.reshape(batch_size, down_count, 8, across_count, 8, last_dim)
        return shaped.transpose(0, 1, 3, 2, 4, 5).reshape(batch_size, window_count, 64, last_dim)

    query_win = to_windows(queries)
    pair_win = to_windows(pair_cells)
    grid_rows = (row_start + jnp.arange(row_count, dtype=jnp.int32)) % lat_cells
    region = row_region(grid_rows, lat_cells).reshape(down_count, 8)
    region = jnp.broadcast_to(region[:, None, :, None], (down_count, across_count, 8, 8)).reshape(
        window_count, 64
    )
    sea_tiled = jnp.tile(sea_mask, (2, 2))
    sea_keep = lax.dynamic_slice(
        sea_tiled, (row_start % lat_cells, col_start % lon_cells), (row_count, col_count)
    )
    sea_keep = (
        sea_keep.reshape(down_count, 8, across_count, 8)
        .transpose(0, 2, 1, 3)
        .reshape(window_count, 64)
        == 1
    )
    same_cell = jnp.eye(64, dtype=bool)
    allowed = (region[:, :, None] == region[:, None, :]) & (sea_keep[:, None, :] | same_cell[None])
    group_width = 4 * head_size
    score_scale = head_size ** (-0.5)

    def one_group(group_index):
        first_col = group_index * group_width
        split_shape = (batch_size, window_count, 64, 4, head_size)
        query_part = lax.dynamic_slice_in_dim(query_win, first_col, group_width, 3).reshape(
            split_shape
        )
        key_part = lax.dynamic_slice_in_dim(pair_win, first_col, group_width, 3).reshape(
            split_shape
        )
        value_part = lax.dynamic_slice_in_dim(
            pair_win, feat_width + first_col, group_width, 3
        ).reshape(split_shape)
        bias_part = lax.dynamic_slice_in_dim(pos_bias, group_index * 4, 4, 0)
        scores = jnp.einsum(
            "bsqhd,bskhd->bshqk", query_part, key_part, preferred_element_type=jnp.float32
        )
        scores = scores * score_scale + bias_part[None, None]
        scores = jnp.where(allowed[None, :, None], scores, -1e30)
        row_top = jnp.max(scores, axis=-1, keepdims=True)
        weights = jnp.exp(scores - row_top)
        attn_probs = (weights / jnp.sum(weights, axis=-1, keepdims=True)).astype(jnp.bfloat16)
        context = jnp.einsum(
            "bshqk,bskhd->bsqhd", attn_probs, value_part, preferred_element_type=jnp.float32
        )
        return context.astype(jnp.bfloat16).reshape(batch_size, window_count, 64, group_width)

    groups = lax.map(one_group, jnp.arange(head_count // 4, dtype=jnp.int32))
    context = jnp.transpose(groups, (1, 2, 3, 0, 4)).reshape(
        batch_size, down_count, across_count, 8, 8, feat_width
    )
    return context.transpose(0, 1, 3, 2, 4, 5).reshape(batch_size, row_count, col_count, feat_width)


def per_device(tokens, qkv_weight, proj_weight, up_weight, down_weight, bias_table, sea_mask):
    batch_size, lat_rows, lon_cols, feat_width = tokens.shape
    head_count = bias_table.shape[1]
    row_base = ((lax.axis_index("zl") * 4 + lax.axis_index("y")) * 2 + lax.axis_index("c")) * lat_rows
    col_base = (lax.axis_index("zh") * 4 + lax.axis_index("x")) * lon_cols
    offset_ids = offsets_table().reshape(-1)
    one_hot = (
        offset_ids[:, None] == jnp.arange(bias_table.shape[0], dtype=jnp.int32)[None, :]
    ).astype(jnp.float32)
    pos_bias = jnp.dot(one_hot, bias_table, precision=lax.Precision.HIGHEST)
    pos_bias = pos_bias.reshape(64, 64, head_count).transpose(2, 0, 1)
    qkv_all, proj_all, up_part, down_part = gather_weights(
        (qkv_weight, proj_weight, up_weight, down_weight)
    )
    normed = layer_norm(tokens)
    arrived = from_behind(normed[:, :4], LAT, -1)
    rolled_rows = jnp.concatenate([normed[:, 4:], arrived], axis=1)
    arrived_cols = from_behind(rolled_rows[:, :, :4], LON, -1)
    feed_cells = jnp.concatenate([rolled_rows[:, :, 4:], arrived_cols], axis=2)
    feed_flat = feed_cells.reshape(-1, feat_width)
    projected = lax.dot_general(
        feed_flat,
        qkv_all,
        (((1,), (1,)), ((), ())),
        preferred_element_type=jnp.float32,
    ).astype(jnp.bfloat16)
    projected = projected.reshape(batch_size, lat_rows, lon_cols, 3 * feat_width)
    queries = projected[..., :feat_width]
    pair_cells = projected[..., feat_width:]
    rolled_context = window_attention(
        queries, pair_cells, row_base + 4, col_base + 4, sea_mask, pos_bias
    )
    came_cols = from_behind(rolled_context[:, :, lon_cols - 4 :], LON, 1)
    back_cols = jnp.concatenate([came_cols, rolled_context[:, :, : lon_cols - 4]], axis=2)
    came_rows = from_behind(back_cols[:, lat_rows - 4 :], LAT, 1)
    context = jnp.concatenate([came_rows, back_cols[:, : lat_rows - 4]], axis=1)
    context_flat = context.reshape(-1, feat_width)
    attention_out = lax.dot_general(
        context_flat,
        proj_all,
        (((1,), (1,)), ((), ())),
        preferred_element_type=jnp.float32,
    )
    attended = (tokens.reshape(-1, feat_width).astype(jnp.float32) + attention_out).astype(
        jnp.bfloat16
    )
    normed_two = layer_norm(attended)
    hidden = lax.dot_general(
        normed_two, up_part, (((1,), (1,)), ((), ())), preferred_element_type=jnp.float32
    )
    hidden = jax.nn.gelu(hidden).astype(jnp.bfloat16)
    hidden_sum = jnp.dot(hidden, down_part, preferred_element_type=jnp.float32)
    result = (attended.astype(jnp.float32) + hidden_sum).astype(jnp.bfloat16)
    return result.reshape(tokens.shape)


def solution(mesh):
    torus = Mesh(mesh.devices.reshape(SIZES), AXES)
    rows = P(LAT + LON, None)
    return jax.shard_map(
        per_device,
        mesh=torus,
        in_specs=(P(None, LAT, LON, None), rows, rows, rows, rows, P(), P()),
        out_specs=P(None, LAT, LON, None),
        check_vma=False,
    )
```

```python
import jax
import jax.numpy as jnp
from jax import lax
from jax.experimental import pallas as pl
from jax.experimental.pallas import tpu as pltpu
from jax.sharding import Mesh
from jax.sharding import PartitionSpec as P

BF = jnp.bfloat16
F32 = jnp.float32
NT = (((1,), (1,)), ((), ()))
VMEM_LIMIT = 60 * 1024 * 1024


def block_copies(src, dst, first, count, sem):
    copies = []
    for zl in range(2):
        for y in range(4):
            for c in range(2):
                for zh in range(2):
                    copies.append(
                        pltpu.make_async_copy(
                            src.at[zh, zl, y, :, c, pl.ds(first, count), :],
                            dst.at[zl, y, c, zh],
                            sem,
                        )
                    )
    return copies


def attention_kernel(x_ref, every_ref, bias_ref, mask_ref, out_ref, w_ref, xw_ref, qkv_ref, sem):
    samples = x_ref.shape[0]

    @pl.when(pl.program_id(0) == 0)
    def _():
        for copy in block_copies(every_ref, w_ref, 0, 24, sem):
            copy.start()

    for s in range(samples):
        for w in range(4):
            xw_ref[pl.ds((s * 4 + w) * 64, 64), :] = x_ref[s, :, w].reshape(64, 1024)

    @pl.when(pl.program_id(0) == 0)
    def _():
        pltpu.make_async_copy(w_ref, w_ref, sem).wait()

    weights = w_ref.reshape(3072, 1024)
    for n in range(6):
        y = lax.dot_general(
            xw_ref[...], weights[pl.ds(n * 512, 512), :], NT, preferred_element_type=F32
        )
        if n < 2:
            y = y * 0.125
        qkv_ref[:, pl.ds(n * 512, 512)] = y.astype(BF)

    low = lax.broadcasted_iota(jnp.int32, (128, 128), 1) < 64
    zero = jnp.zeros((128, 128), BF)
    ones = jnp.ones((128, 128), BF)

    @pl.loop(0, samples * 2)
    def _(pair):
        rows = pl.ds(pl.multiple_of(pair * 128, 128), 128)
        sample, half = pair // 2, pair % 2
        mask = mask_ref[half]
        for j in range(8):
            q = qkv_ref[rows, pl.ds(j * 128, 128)]
            k = qkv_ref[rows, pl.ds(1024 + j * 128, 128)]
            v = qkv_ref[rows, pl.ds(2048 + j * 128, 128)]
            both = jnp.concatenate([jnp.where(low, q, zero), jnp.where(low, zero, q)], axis=0)
            scores = lax.dot_general(both, k, NT, preferred_element_type=F32)
            scores = scores.reshape(2, 128, 128) + bias_ref[pl.ds(2 * j, 2)] + mask[None]
            scores = scores.reshape(256, 128)
            top = jnp.max(scores, axis=-1, keepdims=True)
            probs = jnp.exp(scores - top).astype(BF)
            summed = jnp.dot(probs, jnp.concatenate([v, ones], axis=1), preferred_element_type=F32)
            context = summed[:, :128] / summed[:, 128:]
            context = jnp.where(low, context[:128], context[128:]).astype(BF)
            for i in range(2):
                out_ref[sample, :, half * 2 + i, :, pl.ds(j * 128, 128)] = context[
                    i * 64 : (i + 1) * 64
                ].reshape(8, 8, 128)


def attention(feed, every, bias, mask, step=2):
    batch = feed.shape[0]
    width = 1024
    tokens = step * 256
    return pl.pallas_call(
        attention_kernel,
        grid=(batch // step,),
        in_specs=[
            pl.BlockSpec((step, 8, 4, 8, width), lambda i: (i, 0, 0, 0, 0)),
            pl.BlockSpec(memory_space=pl.ANY),
            pl.BlockSpec((16, 128, 128), lambda i: (0, 0, 0)),
            pl.BlockSpec((2, 128, 128), lambda i: (0, 0, 0)),
        ],
        out_specs=pl.BlockSpec((step, 8, 4, 8, width), lambda i: (i, 0, 0, 0, 0)),
        out_shape=jax.ShapeDtypeStruct((batch, 8, 4, 8, width), BF),
        scratch_shapes=[
            pltpu.VMEM((2, 4, 2, 2, 4, 24, width), BF),
            pltpu.VMEM((tokens, width), BF),
            pltpu.VMEM((tokens, 3 * width), BF),
            pltpu.SemaphoreType.DMA,
        ],
        compiler_params=pltpu.CompilerParams(
            dimension_semantics=("arbitrary",), vmem_limit_bytes=VMEM_LIMIT
        ),
        cost_estimate=pl.CostEstimate(
            flops=2 * batch * 256 * width * 3 * width,
            bytes_accessed=12 << 20,
            transcendentals=batch * 256 * 1024,
        ),
        name="attention",
    )(feed, every, bias, mask)


def normed_rows(values):
    wide = values.astype(F32)
    centre = jnp.mean(wide, axis=-1, keepdims=True)
    shifted = wide - centre
    spread = jnp.mean(shifted * shifted, axis=-1, keepdims=True)
    return (shifted * lax.rsqrt(spread + 1e-05)).astype(BF)


def gelu(x):
    inner = x * (0.7978845608028654 + 0.035677408136300125 * (x * x))
    half = 0.5 * x
    return half + half * jnp.tanh(inner)


def tail_kernel(ctx_ref, tok_ref, every_ref, up_ref, down_ref, out_ref, w_ref, n_ref, acc_ref, sem):
    step = pl.program_id(0)
    rows = ctx_ref.shape[0]
    tile = 256

    @pl.when(step == 0)
    def _():
        for copy in block_copies(every_ref, w_ref, 24, 8, sem):
            copy.start()
        pltpu.make_async_copy(w_ref, w_ref, sem).wait()
        for m in range(rows // tile):
            at = pl.ds(m * tile, tile)
            out = lax.dot_general(
                ctx_ref[at, :], w_ref.reshape(1024, 1024)[...], NT, preferred_element_type=F32
            )
            attended = (tok_ref[at, :].astype(F32) + out).astype(BF)
            acc_ref[at, :] = attended.astype(F32)
            n_ref[at, :] = normed_rows(attended)

    up = up_ref[...].reshape(-1, 1024)
    down = down_ref[...].reshape(-1, 1024)
    for m in range(rows // tile):
        at = pl.ds(m * tile, tile)
        hidden = lax.dot_general(n_ref[at, :], up, NT, preferred_element_type=F32)
        hidden = gelu(hidden).astype(BF)
        acc_ref[at, :] += jnp.dot(hidden, down, preferred_element_type=F32)

    @pl.when(step == pl.num_programs(0) - 1)
    def _():
        out_ref[...] = acc_ref[...].astype(BF)


def tail(context, tokens, every, blocks=16):
    rows, width = context.shape
    flat = every.reshape(128, 96, width)
    whole = lambda i: (0, 0)
    return pl.pallas_call(
        tail_kernel,
        grid=(128 // blocks,),
        in_specs=[
            pl.BlockSpec((rows, width), whole),
            pl.BlockSpec((rows, width), whole),
            pl.BlockSpec(memory_space=pl.ANY),
            pl.BlockSpec((blocks, 32, width), lambda i: (i, 1, 0)),
            pl.BlockSpec((blocks, 32, width), lambda i: (i, 2, 0)),
        ],
        out_specs=pl.BlockSpec((rows, width), whole),
        out_shape=jax.ShapeDtypeStruct((rows, width), BF),
        scratch_shapes=[
            pltpu.VMEM((2, 4, 2, 2, 4, 8, width), BF),
            pltpu.VMEM((rows, width), BF),
            pltpu.VMEM((rows, width), F32),
            pltpu.SemaphoreType.DMA,
        ],
        compiler_params=pltpu.CompilerParams(
            dimension_semantics=("arbitrary",), vmem_limit_bytes=VMEM_LIMIT
        ),
        cost_estimate=pl.CostEstimate(
            flops=2 * rows * width * 9 * width,
            bytes_accessed=24 << 20,
            transcendentals=rows * 4096,
        ),
        name="tail",
    )(context, tokens, every, flat, flat)


AXES = ("zl", "y", "c", "zh", "x")
SIZES = (2, 4, 2, 2, 4)
LAT = ("zl", "y", "c")
LON = ("zh", "x")
TORUS = ("zh", "zl", "y", "x", "c")


def shifted(value, down, right):
    if right == 0:
        return lax.ppermute(value, LAT, [(i, (i + down) % 16) for i in range(16)])
    if down == 0:
        return lax.ppermute(value, LON, [(j, (j + right) % 8) for j in range(8)])
    pairs = [
        (i * 8 + j, (i + down) % 16 * 8 + (j + right) % 8) for i in range(16) for j in range(8)
    ]
    return lax.ppermute(value, AXES, pairs)


def layer_norm(values):
    widened = values.astype(F32)
    centre = jnp.mean(widened, axis=-1, keepdims=True)
    spread = jnp.mean(jnp.square(widened - centre), axis=-1, keepdims=True)
    return ((widened - centre) * lax.rsqrt(spread + 1e-05)).astype(BF)


def position_bias(bias_table):
    cell_ids = jnp.arange(64, dtype=jnp.int32)
    row_of, col_of = cell_ids // 8, cell_ids % 8
    offsets = (row_of[:, None] - row_of[None, :] + 7) * 15 + (col_of[:, None] - col_of[None, :] + 7)
    one_hot = (
        offsets.reshape(-1)[:, None] == jnp.arange(bias_table.shape[0], dtype=jnp.int32)[None, :]
    ).astype(F32)
    pos_bias = jnp.dot(one_hot, bias_table, precision=lax.Precision.HIGHEST)
    pos_bias = pos_bias.reshape(64, 64, bias_table.shape[1]).transpose(2, 0, 1)
    return jnp.tile(pos_bias, (1, 2, 2))


def window_mask(sea_mask, row_start, col_start):
    sea = lax.dynamic_slice(
        jnp.tile(sea_mask, (2, 2)), (row_start % 128, col_start % 256), (8, 32)
    )
    sea = sea.reshape(8, 4, 8).transpose(1, 0, 2).reshape(4, 64) == 1
    rows = (row_start + jnp.arange(8, dtype=jnp.int32)) % 128
    region = jnp.repeat(jnp.where(rows < 4, 2, jnp.where(rows >= 124, 1, 0)), 8)
    same_cell = jnp.eye(64, dtype=bool)
    allowed = (region[:, None] == region[None, :])[None] & (sea[:, None, :] | same_cell[None])
    allowed = allowed.reshape(2, 2, 64, 1, 64) & jnp.eye(2, dtype=bool)[None, :, None, :, None]
    return jnp.where(allowed, 0.0, -1e30).astype(F32).reshape(2, 128, 128)


def per_device(tokens, qkv_weight, proj_weight, up_weight, down_weight, bias_table, sea_mask):
    row_base = ((lax.axis_index("zl") * 4 + lax.axis_index("y")) * 2 + lax.axis_index("c")) * 8
    col_base = (lax.axis_index("zh") * 4 + lax.axis_index("x")) * 32
    shards = jnp.concatenate([qkv_weight, proj_weight, up_weight, down_weight], axis=0)
    every = lax.all_gather(shards, TORUS, axis=0, tiled=True).reshape(2, 2, 4, 4, 2, 96, 1024)
    bias = position_bias(bias_table)
    mask = window_mask(sea_mask, row_base + 4, col_base + 4)
    normed = layer_norm(tokens)
    low = shifted(normed[:, :4, 4:], -1, 0)
    right = shifted(normed[:, 4:, :4], 0, -1)
    corner = shifted(normed[:, :4, :4], -1, -1)
    feed = jnp.concatenate(
        [
            jnp.concatenate([normed[:, 4:, 4:], right], axis=2),
            jnp.concatenate([low, corner], axis=2),
        ],
        axis=1,
    )
    context = attention(feed.reshape(4, 8, 4, 8, 1024), every, bias, mask).reshape(4, 8, 32, 1024)
    up = shifted(context[:, 4:, :28], 1, 0)
    left = shifted(context[:, :4, 28:], 0, 1)
    corner = shifted(context[:, 4:, 28:], 1, 1)
    context = jnp.concatenate(
        [
            jnp.concatenate([corner, up], axis=2),
            jnp.concatenate([left, context[:, :4, :28]], axis=2),
        ],
        axis=1,
    )
    out = tail(context.reshape(-1, 1024), tokens.reshape(-1, 1024), every)
    return out.reshape(tokens.shape)


def solution(mesh):
    torus = Mesh(mesh.devices.reshape(SIZES), AXES)
    rows = P(LAT + LON, None)
    return jax.shard_map(
        per_device,
        mesh=torus,
        in_specs=(P(None, LAT, LON, None), rows, rows, rows, rows, P(), P()),
        out_specs=P(None, LAT, LON, None),
        check_vma=False,
    )
```

```python
import jax
import jax.numpy as jnp
from jax import lax
from jax.experimental import pallas as pl
from jax.experimental.pallas import tpu as pltpu
from jax.sharding import Mesh
from jax.sharding import PartitionSpec as P

BF = jnp.bfloat16
F32 = jnp.float32
NT = (((1,), (1,)), ((), ()))
VMEM_LIMIT = 60 * 1024 * 1024

AXES = ("zl", "y", "c", "zh", "x")
SIZES = (2, 4, 2, 2, 4)
LAT = ("zl", "y", "c")
LON = ("zh", "x")
TORUS = ("zh", "zl", "y", "x", "c")


def behind(at, k):
    return (at + jnp.where(k == 0, 0, jnp.where(k == 1, 3, jnp.where(k == 2, 1, 2)))) % 4


def normed_rows(values):
    wide = values.astype(F32)
    centre = jnp.mean(wide, axis=-1, keepdims=True)
    shifted = wide - centre
    spread = jnp.mean(shifted * shifted, axis=-1, keepdims=True)
    return (shifted * lax.rsqrt(spread + 1e-05)).astype(BF)


ANYWHERE = pl.BlockSpec(memory_space=pl.ANY)
IN_VMEM = pl.BlockSpec(memory_space=pltpu.VMEM)
IN_SMEM = pl.BlockSpec(memory_space=pltpu.SMEM)


def normed_kernel(tok_ref, norm_ref, low_ref, right_ref, corner_ref):
    normed = normed_rows(tok_ref[0].reshape(256, 1024)).reshape(8, 32, 1024)
    norm_ref[0] = normed
    low_ref[0] = normed[:4]
    right_ref[0] = normed[4:, :4]
    corner_ref[0] = normed[:4, :4]


def normed_pieces(tokens):
    batch, width = tokens.shape[0], tokens.shape[3]
    shapes = [(8, 32), (4, 32), (4, 4), (4, 4)]
    spec = lambda shape: pl.BlockSpec((1, *shape, width), lambda i: (i, 0, 0, 0))
    return pl.pallas_call(
        normed_kernel,
        grid=(batch,),
        in_specs=[spec((8, 32))],
        out_specs=[spec(shape) for shape in shapes],
        out_shape=[jax.ShapeDtypeStruct((batch, *shape, width), BF) for shape in shapes],
        compiler_params=pltpu.CompilerParams(
            dimension_semantics=("arbitrary",), vmem_limit_bytes=16 << 20
        ),
        cost_estimate=pl.CostEstimate(flops=60 << 20, bytes_accessed=5 << 20, transcendentals=0),
        name="normed",
    )(tokens)


def first_pack_kernel(place_ref, a0, a1, a2, a3, b0, b1, b2, b3, a_ref, b_ref):
    for k, (a, b) in enumerate(((a0, b0), (a1, b1), (a2, b2), (a3, b3))):
        a_ref[behind(place_ref[0], k)] = a[...]
        b_ref[behind(place_ref[1], k)] = b[...]


def second_pack_kernel(place_ref, a0, a1, a2, a3, b0, b1, b2, b3, a_ref, b_ref):
    for k, (a, b) in enumerate(((a0, b0), (a1, b1), (a2, b2), (a3, b3))):
        z = behind(place_ref[2], k)
        a_ref[behind(place_ref[1], k)] = a[...]
        for y in range(4):
            b_ref[z % 2, y, z // 2] = b[y]


def packed(kernel, place, a, b, a_shape, b_shape):
    return pl.pallas_call(
        kernel,
        in_specs=[IN_SMEM] + [IN_VMEM] * 8,
        out_specs=[IN_VMEM] * 2,
        out_shape=[jax.ShapeDtypeStruct(a_shape, BF), jax.ShapeDtypeStruct(b_shape, BF)],
        compiler_params=pltpu.CompilerParams(vmem_limit_bytes=16 << 20),
        cost_estimate=pl.CostEstimate(flops=1 << 20, bytes_accessed=2 << 20, transcendentals=0),
        name="packed",
    )(place, *a, *b)


def attention_kernel(place_ref, norm_ref, low_ref, right_ref, corner_ref, bias_ref, sea_ref, *refs):
    a_refs, b_refs = refs[:8], refs[8:16]
    top_out, low_out, right_out, corner_out, proj_out = refs[16:21]
    w_ref, feed_ref, xw_ref, qkv_ref, add_ref, sem, proj_sem = refs[21:]
    samples = norm_ref.shape[0]
    for n in range(8):
        c = place_ref[3] if n < 4 else 1 - place_ref[3]
        z = behind(place_ref[2], n % 4)
        x = behind(place_ref[0], n % 4)
        pltpu.make_async_copy(
            a_refs[n], w_ref.at[z % 2, :, c, z // 2, :, pl.ds(0, 16)], sem
        ).start()
        for zl in range(2):
            pltpu.make_async_copy(
                b_refs[n].at[zl, :, :, pl.ds(0, 8)], w_ref.at[zl, :, c, :, x, pl.ds(16, 8)], sem
            ).start()
            pltpu.make_async_copy(
                b_refs[n].at[zl, :, :, pl.ds(8, 8)], proj_out.at[zl, :, c, :, x], proj_sem
            ).start()

    query = lax.broadcasted_iota(jnp.int32, (128, 128), 0)
    key = lax.broadcasted_iota(jnp.int32, (128, 128), 1)
    near = (query // 64 == key // 64) & (
        (query % 64 // 32 == key % 64 // 32) | jnp.broadcast_to(place_ref[4] == 0, (128, 128))
    )
    for half in range(2):
        allowed = near & ((sea_ref[half] == 1) | (query == key))
        for h in range(16):
            bias = bias_ref[h]
            bias = jnp.concatenate([bias, bias], axis=1)
            bias = jnp.concatenate([bias, bias], axis=0)
            add_ref[half, h] = jnp.where(allowed, bias, -1e30)

    for s in range(samples):
        feed_ref[:4, :28] = norm_ref[s, 4:, 4:]
        feed_ref[:4, 28:] = right_ref[s]
        feed_ref[4:, :28] = low_ref[s, :, 4:]
        feed_ref[4:, 28:] = corner_ref[s]
        for w in range(4):
            xw_ref[pl.ds((s * 4 + w) * 64, 64), :] = feed_ref[:, w * 8 : w * 8 + 8].reshape(64, 1024)
    pltpu.make_async_copy(w_ref, w_ref, sem).wait()

    weights = w_ref.reshape(3072, 1024)

    @pl.loop(0, 6)
    def _(n):
        at = pl.ds(pl.multiple_of(n * 512, 512), 512)
        y = lax.dot_general(xw_ref[...], weights[at, :], NT, preferred_element_type=F32)
        qkv_ref[:, at] = (y * jnp.where(n < 2, 0.125, 1.0)).astype(BF)

    left = lax.broadcasted_iota(jnp.int32, (128, 128), 1) < 64
    zero = jnp.zeros((128, 128), BF)
    ones = jnp.ones((128, 128), BF)

    @pl.loop(0, samples)
    def _(sample):
        for half in range(2):
            rows = pl.ds(pl.multiple_of(sample * 256, 256) + half * 128, 128)
            for j in range(8):
                lanes = pl.ds(j * 128, 128)
                q = qkv_ref[rows, pl.ds(j * 128, 128)]
                k = qkv_ref[rows, pl.ds(1024 + j * 128, 128)]
                v = qkv_ref[rows, pl.ds(2048 + j * 128, 128)]
                both = jnp.concatenate([jnp.where(left, q, zero), jnp.where(left, zero, q)], axis=0)
                scores = lax.dot_general(both, k, NT, preferred_element_type=F32)
                scores = scores + add_ref[half, pl.ds(2 * j, 2)].reshape(256, 128)
                highest = jnp.max(scores, axis=-1, keepdims=True)
                probs = jnp.exp(scores - highest).astype(BF)
                summed = jnp.dot(
                    probs, jnp.concatenate([v, ones], axis=1), preferred_element_type=F32
                )
                total = jnp.where(left, summed[:128, 128:], summed[128:, 128:])
                context = jnp.where(left, summed[:128, :128], summed[128:, :128])
                context = (context / total).astype(BF)
                for i in range(2):
                    block = context[i * 64 : (i + 1) * 64].reshape(8, 8, 128)
                    top_out[sample, :, half * 2 + i, :, lanes] = block[:4]
                    low_out[sample, :, half * 2 + i, :, lanes] = block[4:]
                    if half == 1 and i == 1:
                        right_out[sample, :, :, lanes] = block[:4, 4:]
                        corner_out[sample, :, :, lanes] = block[4:, 4:]

    pltpu.make_async_copy(proj_out, proj_out, proj_sem).wait()


def attention(place, pieces, bias, sea, a, b):
    batch, width = pieces[0].shape[0], 1024
    tokens = batch * 256
    return pl.pallas_call(
        attention_kernel,
        in_specs=[IN_SMEM] + [IN_VMEM] * 6 + [ANYWHERE] * 16,
        out_specs=[IN_VMEM] * 5,
        out_shape=[
            jax.ShapeDtypeStruct((batch, 4, 4, 8, width), BF),
            jax.ShapeDtypeStruct((batch, 4, 4, 8, width), BF),
            jax.ShapeDtypeStruct((batch, 4, 4, width), BF),
            jax.ShapeDtypeStruct((batch, 4, 4, width), BF),
            jax.ShapeDtypeStruct((2, 4, 2, 2, 4, 8, width), BF),
        ],
        scratch_shapes=[
            pltpu.VMEM((2, 4, 2, 2, 4, 24, width), BF),
            pltpu.VMEM((8, 32, width), BF),
            pltpu.VMEM((tokens, width), BF),
            pltpu.VMEM((tokens, 3 * width), BF),
            pltpu.VMEM((2, 16, 128, 128), F32),
            pltpu.SemaphoreType.DMA,
            pltpu.SemaphoreType.DMA,
        ],
        compiler_params=pltpu.CompilerParams(vmem_limit_bytes=VMEM_LIMIT),
        cost_estimate=pl.CostEstimate(
            flops=2 * tokens * width * 4 * width,
            bytes_accessed=12 << 20,
            transcendentals=tokens * 1024,
        ),
        name="attention",
    )(place, *pieces, bias, sea, *a, *b)


def gelu(x):
    inner = x * (0.7978845608028654 + 0.035677408136300125 * (x * x))
    half = 0.5 * x
    return half + half * jnp.tanh(inner)


TILES = 4


def tail_kernel(
    top_ref, low_ref, right_ref, corner_ref, tok_ref, proj_ref, every_ref, out_ref,
    ctx_ref, att_ref, norm_ref, hid_ref, up_ref, down_ref, up_sem, down_sem,
):
    samples = tok_ref.shape[0]
    per, width = 128 // TILES, 4096 // TILES

    def rows_of(t, at, dst, sem):
        blocks = pl.ds(t * per, per)
        return pltpu.make_async_copy(
            every_ref.at[blocks, pl.ds(at, 32)], dst.at[blocks], sem.at[t]
        )

    for t in range(TILES):
        rows_of(t, 0, up_ref, up_sem).start()
    for s in range(samples):
        ctx_ref[s, 4:, 4:, :] = top_ref[s].reshape(4, 32, 1024)[:, :28]
        ctx_ref[s, :4, 4:, :] = low_ref[s].reshape(4, 32, 1024)[:, :28]
        ctx_ref[s, 4:, :4, :] = right_ref[s]
        ctx_ref[s, :4, :4, :] = corner_ref[s]
    for s in range(samples):
        rows = pl.ds(s * 256, 256)
        out = lax.dot_general(
            ctx_ref[s].reshape(256, 1024), proj_ref[...], NT, preferred_element_type=F32
        )
        attended = (tok_ref[s].reshape(256, 1024).astype(F32) + out).astype(BF)
        att_ref[rows, :] = attended
        norm_ref[rows, :] = normed_rows(attended)
    for t in range(TILES):
        rows_of(t, 32, down_ref, down_sem).start()

    @pl.loop(0, TILES)
    def _(t):
        rows_of(t, 0, up_ref, up_sem).wait()
        up = up_ref[pl.ds(t * per, per)].reshape(width, 1024)
        at = pl.ds(pl.multiple_of(t * width, width), width)
        for s in range(samples):
            rows = pl.ds(s * 256, 256)
            hidden = lax.dot_general(norm_ref[rows, :], up, NT, preferred_element_type=F32)
            hid_ref[rows, at] = gelu(hidden).astype(BF)

    for t in range(TILES):
        rows_of(t, 32, down_ref, down_sem).wait()
    down = down_ref.reshape(4096, 1024)

    @pl.loop(0, samples // 2)
    def _(s):
        rows = pl.ds(pl.multiple_of(s * 512, 512), 512)
        out = jnp.dot(hid_ref[rows, :], down[...], preferred_element_type=F32)
        out = (att_ref[rows, :].astype(F32) + out).astype(BF)
        out_ref[pl.ds(s * 2, 2)] = out.reshape(2, 8, 32, 1024)


def tail(pieces, tokens, proj, every):
    samples, width = tokens.shape[0], 1024
    rows = samples * 256
    vmem = lambda *shape: pltpu.VMEM(shape, BF)
    return pl.pallas_call(
        tail_kernel,
        in_specs=[IN_VMEM] * 6 + [ANYWHERE],
        out_specs=IN_VMEM,
        out_shape=jax.ShapeDtypeStruct(tokens.shape, BF),
        scratch_shapes=[
            vmem(samples, 8, 32, width),
            vmem(rows, width),
            vmem(rows, width),
            vmem(rows, 4 * width),
            vmem(128, 32, width),
            vmem(128, 32, width),
            pltpu.SemaphoreType.DMA((TILES,)),
            pltpu.SemaphoreType.DMA((TILES,)),
        ],
        compiler_params=pltpu.CompilerParams(vmem_limit_bytes=VMEM_LIMIT),
        cost_estimate=pl.CostEstimate(
            flops=2 * rows * width * 9 * width,
            bytes_accessed=24 << 20,
            transcendentals=rows * 4096,
        ),
        name="tail",
    )(*pieces, tokens, proj, every)


def along(value, axis, steps):
    if axis == "z":
        index = lambda z: z % 2 * 2 + z // 2
        pairs = [(index(z), index((z + steps) % 4)) for z in range(4)]
        return lax.ppermute(value, ("zl", "zh"), pairs)
    return lax.ppermute(value, axis, [(i, (i + steps) % 4) for i in range(4)])


def ring(value, axis):
    return [value, along(value, axis, 1), along(value, axis, -1), along(value, axis, 2)]


def gathered(place, a, b, early, halo):
    a, b = packed(
        first_pack_kernel, place, ring(a, "x"), ring(b, "y"), (4, 16, 1024), (4, 16, 1024)
    )
    place, early, halo = lax.optimization_barrier((place, early, halo))
    a, b = packed(
        second_pack_kernel, place, ring(a, "y"), ring(b, "z"), (4, 4, 16, 1024), (2, 4, 2, 16, 1024)
    )
    low, right, corner = halo
    a, b = ring(a, "z"), ring(b, "x")
    halo = shifted(low, -1, 0), shifted(right, 0, -1), shifted(corner, -1, -1)
    a[3], halo = lax.optimization_barrier((a[3], halo))
    swap = lambda value: lax.ppermute(value, "c", [(0, 1), (1, 0)])
    return a + [swap(v) for v in a], b + [swap(v) for v in b], early, halo


def shifted(value, down, right):
    if right == 0:
        return lax.ppermute(value, LAT, [(i, (i + down) % 16) for i in range(16)])
    if down == 0:
        return lax.ppermute(value, LON, [(j, (j + right) % 8) for j in range(8)])
    pairs = [
        (i * 8 + j, (i + down) % 16 * 8 + (j + right) % 8) for i in range(16) for j in range(8)
    ]
    return lax.ppermute(value, AXES, pairs)


def position_bias(bias_table):
    cell_ids = jnp.arange(64, dtype=jnp.int32)
    row_of, col_of = cell_ids // 8, cell_ids % 8
    offsets = (row_of[:, None] - row_of[None, :] + 7) * 15 + (col_of[:, None] - col_of[None, :] + 7)
    one_hot = (
        jnp.arange(bias_table.shape[0], dtype=jnp.int32)[:, None] == offsets.reshape(-1)[None, :]
    ).astype(F32)
    pos_bias = jnp.dot(bias_table.T, one_hot, precision=lax.Precision.HIGHEST)
    return pos_bias.reshape(bias_table.shape[1], 64, 64)


def window_sea(sea_mask, row_start, col_start):
    sea = lax.dynamic_slice(
        jnp.tile(sea_mask, (2, 2)), (row_start % 128, col_start % 256), (8, 32)
    )
    return sea.reshape(8, 4, 8).transpose(1, 0, 2).reshape(2, 1, 128)


def per_device(tokens, qkv_weight, proj_weight, up_weight, down_weight, bias_table, sea_mask):
    x, y, core = lax.axis_index("x"), lax.axis_index("y"), lax.axis_index("c")
    zh, zl = lax.axis_index("zh"), lax.axis_index("zl")
    strip = (zl * 4 + y) * 2 + core
    place = jnp.stack([x, y, zh * 2 + zl, core, strip == 15]).astype(jnp.int32)
    shards = jnp.concatenate([up_weight, down_weight], axis=0)
    every = lax.all_gather(shards, TORUS, axis=0, tiled=True).reshape(128, 64, 1024)
    bias = position_bias(bias_table)
    sea = window_sea(sea_mask, strip * 8 + 4, (zh * 4 + x) * 32 + 4)
    normed, *halo = normed_pieces(tokens)
    a, b, (bias, sea), halo = gathered(
        place,
        qkv_weight[:16],
        jnp.concatenate([qkv_weight[16:], proj_weight], axis=0),
        (bias, sea),
        tuple(halo),
    )
    pieces = (normed, *halo)
    top, low, right, corner, proj = attention(place, pieces, bias, sea, a, b)
    pieces = (top, shifted(low, 1, 0), shifted(right, 0, 1), shifted(corner, 1, 1))
    return tail(pieces, tokens, proj.reshape(1024, 1024), every)


def solution(mesh):
    torus = Mesh(mesh.devices.reshape(SIZES), AXES)
    rows = P(LAT + LON, None)
    return jax.shard_map(
        per_device,
        mesh=torus,
        in_specs=(P(None, LAT, LON, None), rows, rows, rows, rows, P(), P()),
        out_specs=P(None, LAT, LON, None),
        check_vma=False,
    )
```

```python
import jax
import jax.numpy as jnp
from jax import lax
from jax.experimental import pallas as pl
from jax.experimental.pallas import tpu as pltpu
from jax.sharding import Mesh
from jax.sharding import PartitionSpec as P

BF = jnp.bfloat16
F32 = jnp.float32
NT = (((1,), (1,)), ((), ()))
VMEM_LIMIT = 60 * 1024 * 1024

AXES = ("zl", "y", "c", "zh", "x")
SIZES = (2, 4, 2, 2, 4)
LAT = ("zl", "y", "c")
LON = ("zh", "x")
TORUS = ("zh", "zl", "y", "x", "c")


def behind(at, k):
    return (at + jnp.where(k == 0, 0, jnp.where(k == 1, 3, jnp.where(k == 2, 1, 2)))) % 4


def normed_rows(values):
    wide = values.astype(F32)
    centre = jnp.mean(wide, axis=-1, keepdims=True)
    shifted = wide - centre
    spread = jnp.mean(shifted * shifted, axis=-1, keepdims=True)
    return (shifted * lax.rsqrt(spread + 1e-05)).astype(BF)


ANYWHERE = pl.BlockSpec(memory_space=pl.ANY)
IN_VMEM = pl.BlockSpec(memory_space=pltpu.VMEM)
IN_SMEM = pl.BlockSpec(memory_space=pltpu.SMEM)
IN_HBM = pl.BlockSpec(memory_space=pltpu.HBM)


def normed_kernel(tok_ref, norm_ref, low_ref, right_ref, corner_ref):
    normed = normed_rows(tok_ref[0].reshape(256, 1024)).reshape(8, 32, 1024)
    norm_ref[0] = normed
    low_ref[0] = normed[:4]
    right_ref[0] = normed[4:, :4]
    corner_ref[0] = normed[:4, :4]


def normed_pieces(tokens):
    batch, width = tokens.shape[0], tokens.shape[3]
    shapes = [(8, 32), (4, 32), (4, 4), (4, 4)]
    spec = lambda shape: pl.BlockSpec((1, *shape, width), lambda i: (i, 0, 0, 0))
    return pl.pallas_call(
        normed_kernel,
        grid=(batch,),
        in_specs=[spec((8, 32))],
        out_specs=[spec(shape) for shape in shapes],
        out_shape=[jax.ShapeDtypeStruct((batch, *shape, width), BF) for shape in shapes],
        compiler_params=pltpu.CompilerParams(
            dimension_semantics=("arbitrary",), vmem_limit_bytes=16 << 20
        ),
        cost_estimate=pl.CostEstimate(flops=60 << 20, bytes_accessed=5 << 20, transcendentals=0),
        name="normed",
    )(tokens)


def shards_kernel(qkv_ref, proj_ref, up_ref, down_ref, feed_ref, a_ref, b_ref):
    feed_ref[:32] = up_ref[...]
    feed_ref[32:] = down_ref[...]
    a_ref[...] = qkv_ref[:16]
    b_ref[:8] = qkv_ref[16:]
    b_ref[8:] = proj_ref[...]


def shards(*weights):
    shape = lambda rows: jax.ShapeDtypeStruct((rows, 1024), BF)
    return pl.pallas_call(
        shards_kernel,
        in_specs=[IN_VMEM] * 4,
        out_specs=[IN_VMEM] * 3,
        out_shape=[shape(64), shape(16), shape(16)],
        compiler_params=pltpu.CompilerParams(vmem_limit_bytes=4 << 20),
        cost_estimate=pl.CostEstimate(flops=1 << 16, bytes_accessed=1 << 19, transcendentals=0),
        name="shards",
    )(*weights)


def first_pack_kernel(place_ref, a0, a1, a2, a3, b0, b1, b2, b3, a_ref, b_ref):
    for k, (a, b) in enumerate(((a0, b0), (a1, b1), (a2, b2), (a3, b3))):
        a_ref[behind(place_ref[0], k)] = a[...]
        b_ref[behind(place_ref[1], k)] = b[...]


def second_pack_kernel(place_ref, a0, a1, a2, a3, b0, b1, b2, b3, a_ref, b_ref):
    for k, (a, b) in enumerate(((a0, b0), (a1, b1), (a2, b2), (a3, b3))):
        z = behind(place_ref[2], k)
        a_ref[behind(place_ref[1], k)] = a[...]
        for y in range(4):
            b_ref[z % 2, y, z // 2] = b[y]


def packed(kernel, place, a, b, a_shape, b_shape):
    return pl.pallas_call(
        kernel,
        in_specs=[IN_SMEM] + [IN_VMEM] * 8,
        out_specs=[IN_VMEM] * 2,
        out_shape=[jax.ShapeDtypeStruct(a_shape, BF), jax.ShapeDtypeStruct(b_shape, BF)],
        compiler_params=pltpu.CompilerParams(vmem_limit_bytes=16 << 20),
        cost_estimate=pl.CostEstimate(flops=1 << 20, bytes_accessed=2 << 20, transcendentals=0),
        name="packed",
    )(place, *a, *b)


def feed_kernel(place_ref, norm_ref, low_ref, right_ref, corner_ref, bias_ref, sea_ref, xw_ref, add_ref, feed_ref):
    query = lax.broadcasted_iota(jnp.int32, (128, 128), 0)
    key = lax.broadcasted_iota(jnp.int32, (128, 128), 1)
    near = (query // 64 == key // 64) & (
        (query % 64 // 32 == key % 64 // 32) | jnp.broadcast_to(place_ref[4] == 0, (128, 128))
    )
    for half in range(2):
        allowed = near & ((sea_ref[half] == 1) | (query == key))
        for h in range(16):
            bias = bias_ref[h]
            bias = jnp.concatenate([bias, bias], axis=1)
            bias = jnp.concatenate([bias, bias], axis=0)
            add_ref[half, h] = jnp.where(allowed, bias, -1e30)

    for s in range(norm_ref.shape[0]):
        feed_ref[:4, :28] = norm_ref[s, 4:, 4:]
        feed_ref[:4, 28:] = right_ref[s]
        feed_ref[4:, :28] = low_ref[s, :, 4:]
        feed_ref[4:, 28:] = corner_ref[s]
        for w in range(4):
            xw_ref[pl.ds((s * 4 + w) * 64, 64), :] = feed_ref[:, w * 8 : w * 8 + 8].reshape(64, 1024)


def window_feed(place, pieces, bias, sea):
    width = 1024
    tokens = pieces[0].shape[0] * 256
    return pl.pallas_call(
        feed_kernel,
        in_specs=[IN_SMEM] + [IN_VMEM] * 6,
        out_specs=[IN_VMEM] * 2,
        out_shape=[
            jax.ShapeDtypeStruct((tokens, width), BF),
            jax.ShapeDtypeStruct((2, 16, 128, 128), F32),
        ],
        scratch_shapes=[pltpu.VMEM((8, 32, width), BF)],
        compiler_params=pltpu.CompilerParams(vmem_limit_bytes=24 << 20),
        cost_estimate=pl.CostEstimate(flops=8 << 20, bytes_accessed=8 << 20, transcendentals=0),
        name="feed",
    )(place, *pieces, bias, sea)


def attention_kernel(place_ref, xw_ref, add_ref, *refs):
    a_refs, b_refs = refs[:8], refs[8:16]
    top_out, low_out, right_out, corner_out, proj_out = refs[16:21]
    w_ref, qkv_ref, top_ref, sem, proj_sem, top_sem = refs[21:]
    samples = xw_ref.shape[0] // 256
    for n in range(8):
        c = place_ref[3] if n < 4 else 1 - place_ref[3]
        z = behind(place_ref[2], n % 4)
        x = behind(place_ref[0], n % 4)
        pltpu.make_async_copy(
            a_refs[n], w_ref.at[z % 2, :, c, z // 2, :, pl.ds(0, 16)], sem
        ).start()
        for zl in range(2):
            pltpu.make_async_copy(
                b_refs[n].at[zl, :, :, pl.ds(0, 8)], w_ref.at[zl, :, c, :, x, pl.ds(16, 8)], sem
            ).start()
            pltpu.make_async_copy(
                b_refs[n].at[zl, :, :, pl.ds(8, 8)], proj_out.at[zl, :, c, :, x], proj_sem
            ).start()
    pltpu.make_async_copy(w_ref, w_ref, sem).wait()

    weights = w_ref.reshape(3072, 1024)

    @pl.loop(0, 6, unroll=2)
    def _(n):
        at = pl.ds(pl.multiple_of(n * 512, 512), 512)
        y = lax.dot_general(xw_ref[...], weights[at, :], NT, preferred_element_type=F32)
        qkv_ref[:, at] = (y * jnp.where(n < 2, 0.125, 1.0)).astype(BF)

    left = lax.broadcasted_iota(jnp.int32, (128, 128), 1) < 64
    zero = jnp.zeros((128, 128), BF)
    ones = jnp.ones((128, 128), BF)

    @pl.loop(0, samples)
    def _(sample):
        for half in range(2):
            rows = pl.ds(pl.multiple_of(sample * 256, 256) + half * 128, 128)
            for j in range(8):
                lanes = pl.ds(j * 128, 128)
                q = qkv_ref[rows, pl.ds(j * 128, 128)]
                k = qkv_ref[rows, pl.ds(1024 + j * 128, 128)]
                v = qkv_ref[rows, pl.ds(2048 + j * 128, 128)]
                both = jnp.concatenate([jnp.where(left, q, zero), jnp.where(left, zero, q)], axis=0)
                scores = lax.dot_general(both, k, NT, preferred_element_type=F32)
                scores = scores + add_ref[half, pl.ds(2 * j, 2)].reshape(256, 128)
                highest = jnp.max(scores, axis=-1, keepdims=True)
                probs = jnp.exp(scores - highest).astype(BF)
                summed = jnp.dot(
                    probs, jnp.concatenate([v, ones], axis=1), preferred_element_type=F32
                )
                total = jnp.where(left, summed[:128, 128:], summed[128:, 128:])
                context = jnp.where(left, summed[:128, :128], summed[128:, :128])
                context = (context / total).astype(BF)
                for i in range(2):
                    block = context[i * 64 : (i + 1) * 64].reshape(8, 8, 128)
                    top_ref[sample, :, half * 2 + i, :, lanes] = block[:4]
                    low_out[sample, :, half * 2 + i, :, lanes] = block[4:]
                    if half == 1 and i == 1:
                        right_out[sample, :, :, lanes] = block[:4, 4:]
                        corner_out[sample, :, :, lanes] = block[4:, 4:]

        pltpu.make_async_copy(top_ref.at[sample], top_out.at[sample], top_sem.at[sample]).start()

    pltpu.make_async_copy(proj_out, proj_out, proj_sem).wait()
    for s in range(samples):
        pltpu.make_async_copy(top_ref.at[s], top_out.at[s], top_sem.at[s]).wait()


def attention(place, xw, add, a, b):
    tokens, width = xw.shape
    batch = tokens // 256
    return pl.pallas_call(
        attention_kernel,
        in_specs=[IN_SMEM] + [IN_VMEM] * 2 + [ANYWHERE] * 16,
        out_specs=[IN_HBM] + [IN_VMEM] * 3 + [IN_HBM],
        out_shape=[
            jax.ShapeDtypeStruct((batch, 4, 4, 8, width), BF),
            jax.ShapeDtypeStruct((batch, 4, 4, 8, width), BF),
            jax.ShapeDtypeStruct((batch, 4, 4, width), BF),
            jax.ShapeDtypeStruct((batch, 4, 4, width), BF),
            jax.ShapeDtypeStruct((2, 4, 2, 2, 4, 8, width), BF),
        ],
        scratch_shapes=[
            pltpu.VMEM((2, 4, 2, 2, 4, 24, width), BF),
            pltpu.VMEM((tokens, 3 * width), BF),
            pltpu.VMEM((batch, 4, 4, 8, width), BF),
            pltpu.SemaphoreType.DMA,
            pltpu.SemaphoreType.DMA,
            pltpu.SemaphoreType.DMA((batch,)),
        ],
        compiler_params=pltpu.CompilerParams(vmem_limit_bytes=30 << 20),
        cost_estimate=pl.CostEstimate(
            flops=2 * tokens * width * 4 * width,
            bytes_accessed=12 << 20,
            transcendentals=tokens * 1024,
        ),
        name="attention",
    )(place, xw, add, *a, *b)


def gelu(x):
    inner = x * (0.7978845608028654 + 0.035677408136300125 * (x * x))
    half = 0.5 * x
    return half + half * jnp.tanh(inner)


TILES = 4


def feed_forward(proj_ref, ctx_ref, tok_ref, att_ref, norm_ref, hid_ref, up_ref, down_ref, arrive, store):
    rows = ctx_ref.shape[0]
    per, width = 128 // TILES, 4096 // TILES
    for m in range(2):
        some = pl.ds(m * (rows // 2), rows // 2)
        out = lax.dot_general(ctx_ref[some, :], proj_ref[...], NT, preferred_element_type=F32)
        attended = (tok_ref[some, :].astype(F32) + out).astype(BF)
        att_ref[some, :] = attended
        norm_ref[some, :] = normed_rows(attended)

    @pl.loop(0, TILES)
    def _(t):
        arrive(t)
        up = up_ref[pl.ds(t * per, per)].reshape(width, 1024)
        at = pl.ds(pl.multiple_of(t * width, width), width)
        hidden = lax.dot_general(norm_ref[...], up, NT, preferred_element_type=F32)
        hid_ref[:, at] = gelu(hidden).astype(BF)

    arrive(None)
    down = down_ref.reshape(4096, 1024)

    @pl.loop(0, 2)
    def _(n):
        at = pl.ds(pl.multiple_of(n * 512, 512), 512)
        out = jnp.dot(hid_ref[...], down[:, at], preferred_element_type=F32)
        store(at, (att_ref[:, at].astype(F32) + out).astype(BF))


def inner_kernel(
    top_ref, tok_ref, proj_ref, every_ref, out_ref, up_ref, down_ref,
    ctx_ref, own_ref, att_ref, norm_ref, hid_ref, up_sem, down_sem,
):
    per = 128 // TILES

    def rows_of(t, at, dst, sem):
        blocks = pl.ds(t * per, per)
        return pltpu.make_async_copy(
            every_ref.at[blocks, pl.ds(at, 32)], dst.at[blocks], sem.at[t]
        )

    for t in range(TILES):
        rows_of(t, 0, up_ref, up_sem).start()
    for s in range(4):
        ctx_ref[pl.ds(s * 128, 128), :] = top_ref[s].reshape(128, 1024)
        own_ref[s, :, :28] = tok_ref[s, 4:, 4:]
        own_ref[s, :, 28:] = tok_ref[s, 4:, :4]

    def arrive(t):
        if t is None:
            for n in range(TILES):
                rows_of(n, 32, down_ref, down_sem).wait()
        else:
            rows_of(t, 0, up_ref, up_sem).wait()
            rows_of(t, 32, down_ref, down_sem).start()

    def store(at, out):
        out_ref[:, :, :, at] = out.reshape(4, 4, 32, 512)

    feed_forward(
        proj_ref, ctx_ref, own_ref.reshape(512, 1024), att_ref, norm_ref, hid_ref,
        up_ref, down_ref, arrive, store,
    )


def outer_kernel(
    inner_ref, low_ref, right_ref, corner_ref, tok_ref, proj_ref, up_ref, down_ref, out_ref,
    ctx_ref, own_ref, att_ref, norm_ref, hid_ref,
):
    for s in range(4):
        for r in range(4):
            at = pl.ds(s * 4 + r, 1)
            ctx_ref[at, 4:, :] = low_ref[s, r].reshape(1, 32, 1024)[:, :28]
            ctx_ref[at, :4, :] = corner_ref[s, r].reshape(1, 4, 1024)
            own_ref[at] = tok_ref[s, r].reshape(1, 32, 1024)
            block, first = 16 + (s * 4 + r) // 8, (s * 4 + r) % 8 * 4
            ctx_ref[block, first : first + 4, :] = right_ref[s, r]
            own_ref[block, first : first + 4, :] = tok_ref[s, 4 + r, :4]
        out_ref[s, 4:, 4:] = inner_ref[s, :, :28]

    def store(at, out):
        out = out.reshape(18, 32, 512)
        for s in range(4):
            out_ref[s, :4, :, at] = out[s * 4 : s * 4 + 4]
            for r in range(4):
                block, first = 16 + (s * 4 + r) // 8, (s * 4 + r) % 8 * 4
                out_ref[s, 4 + r, :4, at] = out[block, first : first + 4]

    feed_forward(
        proj_ref, ctx_ref.reshape(576, 1024), own_ref.reshape(576, 1024), att_ref, norm_ref,
        hid_ref, up_ref, down_ref, lambda t: None, store,
    )


def feed_call(kernel, limit, rows, ctx_shape, own_shape, out_shapes, name, *operands):
    width = 1024
    vmem = lambda *shape: pltpu.VMEM(shape, BF)
    first = len(out_shapes) > 1
    return pl.pallas_call(
        kernel,
        in_specs=[IN_VMEM] * (len(operands) - 1) + [ANYWHERE if first else IN_VMEM],
        out_specs=[IN_VMEM] * len(out_shapes),
        out_shape=[jax.ShapeDtypeStruct(shape, BF) for shape in out_shapes],
        scratch_shapes=[
            vmem(*ctx_shape),
            vmem(*own_shape),
            vmem(rows, width),
            vmem(rows, width),
            vmem(rows, 4 * width),
        ]
        + [pltpu.SemaphoreType.DMA((TILES,))] * (2 if first else 0),
        compiler_params=pltpu.CompilerParams(vmem_limit_bytes=limit << 20),
        cost_estimate=pl.CostEstimate(
            flops=2 * rows * width * 9 * width,
            bytes_accessed=22 << 20,
            transcendentals=rows * 4096,
        ),
        name=name,
    )(*operands)


def along(value, axis, steps):
    if axis == "z":
        index = lambda z: z % 2 * 2 + z // 2
        pairs = [(index(z), index((z + steps) % 4)) for z in range(4)]
        return lax.ppermute(value, ("zl", "zh"), pairs)
    return lax.ppermute(value, axis, [(i, (i + steps) % 4) for i in range(4)])


def ring(value, axis):
    return [value, along(value, axis, 1), along(value, axis, -1), along(value, axis, 2)]


def shifted(value, down, right):
    if right == 0:
        return lax.ppermute(value, LAT, [(i, (i + down) % 16) for i in range(16)])
    if down == 0:
        return lax.ppermute(value, LON, [(j, (j + right) % 8) for j in range(8)])
    pairs = [
        (i * 8 + j, (i + down) % 16 * 8 + (j + right) % 8) for i in range(16) for j in range(8)
    ]
    return lax.ppermute(value, AXES, pairs)


def position_bias(bias_table):
    cell_ids = jnp.arange(64, dtype=jnp.int32)
    row_of, col_of = cell_ids // 8, cell_ids % 8
    offsets = (row_of[:, None] - row_of[None, :] + 7) * 15 + (col_of[:, None] - col_of[None, :] + 7)
    one_hot = (
        jnp.arange(bias_table.shape[0], dtype=jnp.int32)[:, None] == offsets.reshape(-1)[None, :]
    ).astype(F32)
    pos_bias = jnp.dot(bias_table.T, one_hot, precision=lax.Precision.HIGHEST)
    return pos_bias.reshape(bias_table.shape[1], 64, 64)


def window_sea(sea_mask, row_start, col_start):
    sea = lax.dynamic_slice(
        jnp.tile(sea_mask, (2, 2)), (row_start % 128, col_start % 256), (8, 32)
    )
    return sea.reshape(8, 4, 8).transpose(1, 0, 2).reshape(2, 1, 128)


def per_device(tokens, qkv_weight, proj_weight, up_weight, down_weight, bias_table, sea_mask):
    x, y, core = lax.axis_index("x"), lax.axis_index("y"), lax.axis_index("c")
    zh, zl = lax.axis_index("zh"), lax.axis_index("zl")
    strip = (zl * 4 + y) * 2 + core
    place = jnp.stack([x, y, zh * 2 + zl, core, strip == 15]).astype(jnp.int32)
    feed_rows, a, b = shards(qkv_weight, proj_weight, up_weight, down_weight)
    every = lax.all_gather(feed_rows, TORUS, axis=0, tiled=True).reshape(128, 64, 1024)
    tied = lax.optimization_barrier
    normed, *halo = normed_pieces(tokens)
    (a, b), halo = tied(((a, b), halo))
    low, right, corner = halo
    halo = shifted(low, -1, 0), shifted(right, 0, -1), shifted(corner, -1, -1)
    a, b = packed(
        first_pack_kernel, place, ring(a, "x"), ring(b, "y"), (4, 16, 1024), (4, 16, 1024)
    )
    a, b, bias_table, sea_mask = tied((a, b, bias_table, sea_mask))
    bias = position_bias(bias_table)
    sea = window_sea(sea_mask, strip * 8 + 4, (zh * 4 + x) * 32 + 4)
    a, b = ring(a, "y"), ring(b, "z")
    b[3], halo, bias, sea = tied((b[3], halo, bias, sea))
    a, b = packed(second_pack_kernel, place, a, b, (4, 4, 16, 1024), (2, 4, 2, 16, 1024))
    place, halo, a, b = tied((place, halo, a, b))
    xw, add = window_feed(place, (normed, *halo), bias, sea)
    a, b = ring(a, "z"), ring(b, "x")
    a[1], xw, add = tied((a[1], xw, add))
    swap = lambda value: lax.ppermute(value, "c", [(0, 1), (1, 0)])
    a, b = a + [swap(v) for v in a], b + [swap(v) for v in b]
    top, low, right, corner, proj = attention(place, xw, add, a, b)
    proj = proj.reshape(1024, 1024)
    low, right, corner = shifted(low, 1, 0), shifted(right, 0, 1), shifted(corner, 1, 1)
    inner, up, down = feed_call(
        inner_kernel, 20, 512, (512, 1024), (4, 4, 32, 1024),
        [(4, 4, 32, 1024), (128, 32, 1024), (128, 32, 1024)], "inner",
        top, tokens, proj, every,
    )
    return feed_call(
        outer_kernel, 26, 576, (18, 32, 1024), (18, 32, 1024), [tokens.shape], "outer",
        inner, low, right, corner, tokens, proj, up, down,
    )[0]


def solution(mesh):
    torus = Mesh(mesh.devices.reshape(SIZES), AXES)
    rows = P(LAT + LON, None)
    return jax.shard_map(
        per_device,
        mesh=torus,
        in_specs=(P(None, LAT, LON, None), rows, rows, rows, rows, P(), P()),
        out_specs=P(None, LAT, LON, None),
        check_vma=False,
    )
```
